32 devices in a mesh: dp: 2 (over x), tp: 16 (over y, z, core).
Axes of the slice: x: 2, y: 2, z: 4, core: 2. Of those that a mesh axis runs over, the one named last changes fastest.
Arguments:
- x: bfloat16 [8192, 4096], P(('dp', 'tp')), parts along dimension 0
- dy: bfloat16 [8192, 4096], P(('dp', 'tp')), parts along dimension 0
- pre: bfloat16 [8192, 16384], P('dp', 'tp'), parts along dimension 0
- w_in: bfloat16 [4096, 16384], P(None, 'tp')
- w_down: bfloat16 [16384, 4096], P('tp')
Outputs:
- output 1: bfloat16 [8192, 4096], P(('dp', 'tp')), parts along dimension 0
- output 2: bfloat16 [8192, 16384], P('dp', 'tp'), parts along dimension 0
- output 3: bfloat16 [32768, 4096], P(('dp', 'tp')), parts along dimension 0
There are 2 independent parts. The reference program is written for one: setup_inputs(seed, part) draws one part's arguments, and reference() takes and returns one part's arrays. A program takes and returns all parts, laid end to end along the dimension named above; an argument that names none is the same for every part.
All inputs are finite; a program needn't handle non-finite values.
Results may differ from the reference program's by a relative error of at most 0.012.
Values are sent between devices in bfloat16 or wider.
A program may use at most 2 GiB of HBM per device.

```python
import jax
import jax.numpy as jnp

ROWS = 4096
D = 4096
FF = 16384


def act(pre):
    return jax.nn.gelu(pre)


def setup_inputs(seed: int = 0, part: int = 0) -> dict:
    kx, ky, ka, ki, kd = jax.random.split(jax.random.key(seed), 5)
    kx, ky, ka = (jax.random.fold_in(k, part) for k in (kx, ky, ka))
    drawn = {
        "x": jax.random.normal(kx, (ROWS, D), jnp.float32),
        "dy": jax.random.normal(ky, (ROWS, D), jnp.float32),
        "pre": jax.random.normal(ka, (ROWS, FF), jnp.float32),
        "w_in": jax.random.normal(ki, (D, FF), jnp.float32) * D**-0.5,
        "w_down": jax.random.normal(kd, (FF, D), jnp.float32) * FF**-0.5,
    }
    return {k: v.astype(jnp.bfloat16) for k, v in drawn.items()}


def reference(x, dy, pre, w_in, w_down):
    hidden, back = jax.vjp(act, pre.astype(jnp.float32))
    d_hidden = jnp.dot(dy, w_down.T, preferred_element_type=jnp.float32)
    d_pre = back(d_hidden)[0].astype(jnp.bfloat16)
    dx = jnp.dot(d_pre, w_in.T, preferred_element_type=jnp.float32)
    dw_in = jnp.dot(x.T, d_pre, preferred_element_type=jnp.float32)
    dw_down = jnp.dot(hidden.astype(jnp.bfloat16).T, dy, preferred_element_type=jnp.float32)
    return tuple(g.astype(jnp.bfloat16) for g in (dx, dw_in, dw_down))
```

```python
import functools

import jax
import jax.numpy as jnp
import numpy as np
from jax import lax
from jax.experimental import pallas as pl
from jax.experimental.pallas import tpu as pltpu
from jax.sharding import PartitionSpec as P

MESH = pl.DeviceIdType.MESH
F32, BF16 = jnp.float32, jnp.bfloat16
D = 4096
FL = 1024
SH = 256
CHUNKS_A = ((0, 48, "p"), (48, 112, "q"), (160, 96, "q"))
CHUNKS_B = ((0, 96, "p"), (96, 80, "q"), (176, 80, "q"))
PR = 96
QR = 160
VMEM = 66_000_000
NT = (((1,), (1,)), ((), ()))
TN = (((0,), (0,)), ((), ()))


def dot(a, b, dims):
    return lax.dot_general(a, b, dims, preferred_element_type=F32)


def where_am_i():
    tp = lax.axis_index("tp")
    return tp // 8, (tp // 2) % 4, tp % 2


def tp_of(y, z, c):
    return y * 8 + z * 2 + c


def rdma(src, dst, ssem, rsem, dev):
    return pltpu.make_async_remote_copy(
        src_ref=src, dst_ref=dst, send_sem=ssem, recv_sem=rsem, device_id={"tp": dev}, device_id_type=MESH
    )


def greet(y, z, c):
    bar = pltpu.get_barrier_semaphore()

    def hello(dev):
        pl.semaphore_signal(bar, inc=1, device_id={"tp": dev}, device_id_type=MESH)

    hello(tp_of(y, z, 1 - c))
    hello(tp_of(1 - y, z, c))

    @pl.when(z > 0)
    def _():
        hello(tp_of(y, z - 1, c))

    @pl.when(z < 3)
    def _():
        hello(tp_of(y, z + 1, c))

    pl.semaphore_wait(bar, 2 + (z + 2) // 3 + (5 - z) // 3)


class Sends:
    def __init__(self):
        self.all = []

    def start(self, pred, make):
        self.all.append((pred, make))
        if pred is None:
            make().start()
        else:
            pl.when(pred)(lambda: make().start())

    def finish(self):
        for pred, make in self.all:
            if pred is None:
                make().wait_send()
            else:
                pl.when(pred)(lambda make=make: make().wait_send())


class Gather:
    def __init__(self, pos, own, full, rsem, zsem, ysem, sib_s, sib_r, chunks):
        self.y, self.z, self.c = pos
        self.own, self.full = own, full
        self.rsem, self.zsem, self.ysem, self.sib_s, self.sib_r = rsem, zsem, ysem, sib_s, sib_r
        self.chunks = chunks
        self.sends = Sends()

    def rows(self, y, z, k, c=None):
        r0, n = (0, SH) if k is None else self.chunks[k][:2]
        off = tp_of(y, z, self.c if c is None else c) * SH + r0
        return self.full.at[pl.ds(pl.multiple_of(off, 16), n)]

    def copy(self, dev, y, z, k, sems, own):
        r0, n, _ = self.chunks[k]
        src = self.own.at[pl.ds(r0, n)] if own else self.rows(y, z, k)
        d = y * 4 + z
        return rdma(src, self.rows(y, z, k), sems.at[d, k], self.rsem.at[d, k], dev)

    def send_z(self, step, y, z, k, pred=None, own=False):
        ok = self.z > 0 if step < 0 else self.z < 3
        if pred is not None:
            ok = jnp.logical_and(ok, pred)
        dev = tp_of(self.y, self.z + step, self.c)
        self.sends.start(ok, lambda: self.copy(dev, y, z, k, self.zsem.at[(step + 1) // 2], own))

    def send_y(self, y, z, k, pred=None, own=False):
        dev = tp_of(1 - self.y, self.z, self.c)
        self.sends.start(pred, lambda: self.copy(dev, y, z, k, self.ysem, own))

    def wait(self, y, z, k):
        self.copy(tp_of(1 - self.y, self.z, self.c), y, z, k, self.ysem, False).wait_recv()

    def sib_copy(self, y, z, c, own=False):
        d = y * 4 + z
        src = self.own if own else self.rows(y, z, None, c)
        return rdma(src, self.rows(y, z, None, c), self.sib_s.at[d], self.sib_r.at[d], tp_of(self.y, self.z, 1 - self.c))

    def send_sib(self, y, z, pred=None, own=False):
        self.sends.start(pred, lambda: self.sib_copy(y, z, self.c, own))

    def wait_sib(self, y, z):
        self.sib_copy(y, z, 1 - self.c).wait_recv()

    def begin(self):
        y, z = self.y, self.z
        for k, (_, _, kind) in enumerate(self.chunks):
            self.send_y(y, z, k, own=True)
            self.send_z(1, y, z, k, own=True)
            self.send_z(-1, y, z, k, own=True)
        self.send_sib(y, z, own=True)

    def turn(self):
        y, z = self.y, self.z
        for k, (_, _, kind) in enumerate(self.chunks):
            if kind == "p":
                self.wait(1 - y, z, k)
                self.send_z(1, 1 - y, z, k)
                self.send_z(-1, 1 - y, z, k)

    def step(self, s):
        y, z = self.y, self.z
        for k, (_, _, kind) in enumerate(self.chunks):
            for side in (-1, 1):
                zs = z + side * (s + 1)
                ok = zs >= 0 if side < 0 else zs <= 3
                for ys in (y, 1 - y) if kind == "p" else (y,):
                    pl.when(ok)(lambda ys=ys, zs=zs, k=k: self.wait(ys, zs, k))
                    if s < 2:
                        self.send_z(-side, ys, zs, k, pred=ok)
                if kind == "q":
                    self.send_y(y, zs, k, pred=ok)
        for side in (-1, 1):
            zs = z + side * (s + 1)
            self.send_sib(y, zs, pred=zs >= 0 if side < 0 else zs <= 3)

    def across(self, s):
        y, z = self.y, self.z
        for side in (-1, 1) if s else (0,):
            zs = z + side * s
            ok = None if s == 0 else zs >= 0 if side < 0 else zs <= 3

            def take(zs=zs):
                for k, (_, _, kind) in enumerate(self.chunks):
                    if kind == "q":
                        self.wait(1 - y, zs, k)

            if ok is None:
                take()
            else:
                pl.when(ok)(take)
            self.send_sib(1 - y, zs, pred=ok)


def local(src, dst, sem):
    return pltpu.make_async_copy(src, dst, sem)


def both(*copies):
    for cp in copies:
        cp.start()
    for cp in copies:
        cp.wait()


def kernel_a(dy, pre, w_down, w_in, full, hidden, dpre, dps, wis,
             wd_v, dy_v, pre_v, hid_v, dp_v, rsem, zsem, ysem, sib_s, sib_r, dps_s, dps_r, wis_sem, lsem):
    y, z, c = where_am_i()
    greet(y, z, c)
    g = Gather((y, z, c), dy, full, rsem, zsem, ysem, sib_s, sib_r, CHUNKS_A)
    g.begin()
    other = tp_of(y, z, 1 - c)
    w_copy = rdma(w_in, wis, wis_sem.at[0], wis_sem.at[1], other)
    w_copy.start()
    load_w = local(w_down, wd_v, lsem.at[4])
    load_w.start()

    def dps_copy(ys, zs):
        off = pl.multiple_of(tp_of(ys, zs, 1 - c) * SH, SH)
        d = ys * 4 + zs
        return rdma(dpre.at[pl.ds(off, SH)], dps.at[pl.ds(pl.multiple_of(d * SH, SH), SH)], dps_s.at[d], dps_r.at[d], other)

    def compute(ys, zs, cs):
        off = pl.multiple_of(tp_of(ys, zs, cs) * SH, SH)
        rows = pl.ds(off, SH)
        both(local(full.at[rows], dy_v, lsem.at[0]), local(pre.at[rows], pre_v, lsem.at[1]))

        def tile(j, _):
            cols = pl.ds(pl.multiple_of(j * 256, 256), 256)
            dh = dot(dy_v[...], wd_v[cols, :], NT)
            p = pre_v[:, cols].astype(F32)
            k = np.float32(np.sqrt(2 / np.pi))
            t = jnp.tanh(k * (p + 0.044715 * (p * p * p)))
            cdf = 0.5 * (1.0 + t)
            slope = cdf + 0.5 * p * (1.0 - t * t) * (k * (1.0 + 3 * 0.044715 * (p * p)))
            hid_v[:, cols] = (p * cdf).astype(BF16)
            dp_v[:, cols] = (dh * slope).astype(BF16)
            return 0

        lax.fori_loop(0, FL // 256, tile, 0)
        both(local(hid_v, hidden.at[rows], lsem.at[2]), local(dp_v, dpre.at[rows], lsem.at[3]))

    def shard(ys, zs, pred=None):
        def go():
            compute(ys, zs, c)
            g.wait_sib(ys, zs)
            compute(ys, zs, 1 - c)
            dps_copy(ys, zs).start()

        if pred is None:
            go()
        else:
            pl.when(pred)(go)

    both(local(dy, dy_v, lsem.at[0]))
    both(local(dy_v, g.rows(y, z, None), lsem.at[0]))
    load_w.wait()
    g.turn()

    def some(s):
        if s == 0:
            shard(y, z)
            g.step(0)
            g.across(0)
            shard(1 - y, z)
            return

        def one(i, _):
            side = 2 * (i // 2) - 1
            zs = z + side * s
            ys = jnp.where(i % 2 == 0, y, 1 - y)
            shard(ys, zs, jnp.logical_and(zs >= 0, zs <= 3))
            return 0

        lax.fori_loop(0, 4, one, 0)

    some(0)
    g.step(1)
    g.across(1)
    some(1)
    g.step(2)
    g.across(2)
    some(2)
    g.across(3)
    some(3)

    for d in range(8):
        cp = rdma(dpre.at[pl.ds(0, SH)], dps.at[pl.ds(d * SH, SH)], dps_s.at[d], dps_r.at[d], other)
        cp.wait_recv()
        cp.wait_send()
    w_copy.wait()
    g.sends.finish()


def kernel_b(x, dy, hidden, dpre, dps, w_in, wis,
             dx, dw_in, dw_down, full, pl_b, pr_b, ps_b, ql_b, qr_b, qs_b, qy_b, qys_b, py_b, pys_b,
             wo_v, ws_v, hid_v, acc, blk, xv, dpv, a1, a2, arr, obuf, tile_o, out_v,
             rsem, zsem, ysem, sib_s, sib_r, p_s, pl_r, pr_r, q_s, ql_r, qr_r, qy_s, qy_r, py_sem, lsem):
    y, z, c = where_am_i()
    greet(y, z, c)
    g = Gather((y, z, c), x, full, rsem, zsem, ysem, sib_s, sib_r, CHUNKS_B)
    g.begin()
    load_wo, load_ws, load_h = (
        local(w_in, wo_v, lsem.at[4]), local(wis, ws_v, lsem.at[5]), local(hidden, hid_v, lsem.at[6]))
    load_wo.start()
    load_ws.start()
    load_h.start()
    sends = Sends()
    left, right = tp_of(y, z - 1, c), tp_of(y, z + 1, c)
    over = tp_of(1 - y, z, c)
    inner = jnp.logical_and(z > 0, z < 3)
    high = z // 2
    far = high * z + (1 - high) * (3 - z)

    def target(i):
        o = (0, 1, 5 - far, far)[i]
        return high * o + (1 - high) * (3 - o)

    def term(ys, zs, r0, n):
        o = pl.multiple_of(tp_of(ys, zs, c) * SH + r0, 16)
        s = pl.multiple_of((ys * 4 + zs) * SH + r0, 16)
        both(local(dpre.at[pl.ds(o, n)], a1.at[pl.ds(0, n)], lsem.at[0]),
             local(dps.at[pl.ds(s, n)], a2.at[pl.ds(0, n)], lsem.at[1]))

        def tile(j, _):
            cols = pl.ds(pl.multiple_of(j * 512, 512), 512)
            blk[0:n, cols] = dot(a1[0:n, :], wo_v[cols, :], NT) + dot(a2[0:n, :], ws_v[cols, :], NT)
            return 0

        lax.fori_loop(0, D // 512, tile, 0)

    def add(buf, wait, n):
        wait()
        both(local(buf, arr.at[pl.ds(0, n)], lsem.at[2]))

        def tile(j, _):
            cols = pl.ds(pl.multiple_of(j * 512, 512), 512)
            blk[0:n, cols] += arr[0:n, cols].astype(F32)
            return 0

        lax.fori_loop(0, D // 512, tile, 0)

    def store(buf, n):
        def tile(j, _):
            cols = pl.ds(pl.multiple_of(j * 512, 512), 512)
            obuf[0:n, cols] = blk[0:n, cols].astype(BF16)
            return 0

        lax.fori_loop(0, D // 512, tile, 0)
        both(local(obuf.at[pl.ds(0, n)], buf, lsem.at[3]))

    def p_copy(ys, v, dev, rightward):
        i = ys * 4 + v
        dst, sem = (pl_b, pl_r) if rightward else (pr_b, pr_r)
        return rdma(ps_b.at[i], dst.at[i], p_s.at[i], sem.at[i], dev)

    def q_copy(v, dev, rightward):
        dst, sem = (ql_b, ql_r) if rightward else (qr_b, qr_r)
        return rdma(qs_b.at[v], dst.at[v], q_s.at[v], sem.at[v], dev)

    def qy_copy(v):
        return rdma(qys_b.at[v], qy_b.at[v], qy_s.at[v], qy_r.at[v], over)

    def py_copy():
        return rdma(pys_b, py_b, py_sem.at[0], py_sem.at[1], over)

    def p_line(i, pred):
        v = target(i)
        up, down = v > z, v < z

        def go():
            for ys in (1 - y, y):
                term(ys, v, 0, PR)
                pl.when(jnp.logical_and(inner, up))(
                    lambda: add(pl_b.at[ys * 4 + v], lambda: p_copy(ys, v, right, True).wait_recv(), PR))
                pl.when(jnp.logical_and(inner, down))(
                    lambda: add(pr_b.at[ys * 4 + v], lambda: p_copy(ys, v, left, False).wait_recv(), PR))
                store(ps_b.at[ys * 4 + v], PR)
                pl.when(up)(lambda: p_copy(ys, v, right, True).start())
                pl.when(down)(lambda: p_copy(ys, v, left, False).start())

        pl.when(pred)(go)

    def q_line(i, pred):
        v = target(i)
        up, down = v > z, v < z

        def go():
            term(y, v, PR, QR)
            add(qy_b.at[v], lambda: qy_copy(v).wait_recv(), QR)
            pl.when(jnp.logical_and(inner, up))(lambda: add(ql_b.at[v], lambda: q_copy(v, right, True).wait_recv(), QR))
            pl.when(jnp.logical_and(inner, down))(lambda: add(qr_b.at[v], lambda: q_copy(v, left, False).wait_recv(), QR))
            store(qs_b.at[v], QR)
            pl.when(up)(lambda: q_copy(v, right, True).start())
            pl.when(down)(lambda: q_copy(v, left, False).start())

        pl.when(pred)(go)

    def towards(i, pred):
        p_line(i, pred)
        q_line(i, pred)

    def p_last(ys):
        term(ys, z, 0, PR)
        i = ys * 4 + z
        pl.when(z > 0)(lambda: add(pl_b.at[i], lambda: p_copy(ys, z, right, True).wait_recv(), PR))
        pl.when(z < 3)(lambda: add(pr_b.at[i], lambda: p_copy(ys, z, left, False).wait_recv(), PR))

    def q_last():
        term(y, z, PR, QR)
        add(qy_b.at[z], lambda: qy_copy(z).wait_recv(), QR)
        pl.when(z > 0)(lambda: add(ql_b.at[z], lambda: q_copy(z, right, True).wait_recv(), QR))
        pl.when(z < 3)(lambda: add(qr_b.at[z], lambda: q_copy(z, left, False).wait_recv(), QR))
        store(dx.at[pl.ds(PR, QR)], QR)

    def down_tiles(first, count):
        def one(j, _):
            cols = pl.ds(pl.multiple_of(j * 512, 512), 512)
            both(local(dy.at[:, cols], tile_o, lsem.at[0]))

            def row(m, _):
                ms = pl.ds(pl.multiple_of(m * 256, 256), 256)
                out_v[ms, :] = dot(hid_v[:, ms], tile_o[...], TN).astype(BF16)
                return 0

            lax.fori_loop(0, FL // 256, row, 0)
            both(local(out_v, dw_down.at[:, cols], lsem.at[0]))
            return 0

        lax.fori_loop(first, first + count, one, 0)

    def in_step(ys, zs):
        rows = pl.ds(pl.multiple_of(tp_of(ys, zs, 0) * SH, SH), 2 * SH)
        both(local(full.at[rows], xv, lsem.at[0]), local(dpre.at[rows], dpv, lsem.at[1]))

        def row(m, _):
            ms = pl.ds(pl.multiple_of(m * 256, 256), 256)
            acc[ms, :] += dot(xv[:, ms], dpv[...], TN)
            return 0

        lax.fori_loop(0, D // 256, row, 0)

    def ready(s):
        def one(i, _):
            side = 2 * (i // 2) - 1
            zs = z + side * s
            ys = jnp.where(i % 2 == 0, y, 1 - y)

            @pl.when(jnp.logical_and(zs >= 0, zs <= 3))
            def _():
                g.wait_sib(ys, zs)
                in_step(ys, zs)

            return 0

        lax.fori_loop(2 if s == 0 else 0, 4, one, 0)

    load_wo.wait()
    load_ws.wait()
    for i in range(4):
        v = target(i)
        term(1 - y, v, PR, QR)
        store(qys_b.at[v], QR)
        qy_copy(v).start()
    g.turn()
    both(local(x, obuf_rows(xv), lsem.at[0]))
    both(local(obuf_rows(xv), g.rows(y, z, None), lsem.at[0]))

    def zero(m, _):
        acc[pl.ds(pl.multiple_of(m * 256, 256), 256), :] = jnp.zeros((256, FL), F32)
        return 0

    lax.fori_loop(0, D // 256, zero, 0)
    load_h.wait()
    outer = jnp.logical_not(inner)
    towards(0, outer)
    down_tiles(0, 2)
    g.step(0)
    g.across(0)
    towards(0, inner)
    ready(0)
    down_tiles(2, 2)
    towards(1, outer)
    g.step(1)
    towards(1, inner)
    g.across(1)
    down_tiles(4, 4)
    towards(2, outer)
    g.step(2)
    towards(2, inner)
    ready(1)
    g.across(2)
    ready(2)
    p_last(1 - y)
    store(pys_b, PR)
    py_copy().start()
    q_last()
    p_last(y)
    add(py_b, lambda: py_copy().wait_recv(), PR)
    store(dx.at[pl.ds(0, PR)], PR)
    g.across(3)
    ready(3)

    def out(m, _):
        ms = pl.ds(pl.multiple_of(m * 512, 512), 512)
        dpv[...] = acc[ms, :].astype(BF16)
        both(local(dpv, dw_in.at[ms], lsem.at[0]))
        return 0

    lax.fori_loop(0, D // 512, out, 0)

    for i in range(3):
        v = target(i)
        for ys in (1 - y, y):
            p_copy(ys, v, left, False).wait_send()
        q_copy(v, left, False).wait_send()
    for i in range(4):
        qy_copy(target(i)).wait_send()
    py_copy().wait_send()
    g.sends.finish()


def obuf_rows(xv):
    return xv.at[pl.ds(0, SH)]


def solution(mesh):
    any_ = pl.BlockSpec(memory_space=pl.ANY)
    dma = pltpu.SemaphoreType.DMA

    def arr(*shape):
        return jax.ShapeDtypeStruct(shape, BF16)

    gather_sems = [dma((8, 3)), dma((2, 8, 3)), dma((8, 3)), dma((8,)), dma((8,))]

    def step(x, dy, pre, w_in, w_down):
        full, hidden, dpre, dps, wis = pl.pallas_call(
            kernel_a,
            name="gather_dy",
            out_shape=[arr(D, D), arr(D, FL), arr(D, FL), arr(8 * SH, FL), arr(D, FL)],
            in_specs=[any_] * 4,
            out_specs=[any_] * 5,
            scratch_shapes=[
                pltpu.VMEM((FL, D), BF16), pltpu.VMEM((SH, D), BF16), pltpu.VMEM((SH, FL), BF16),
                pltpu.VMEM((SH, FL), BF16), pltpu.VMEM((SH, FL), BF16),
                *gather_sems, dma((8,)), dma((8,)), dma((2,)), dma((5,)),
            ],
            compiler_params=pltpu.CompilerParams(collective_id=0, has_side_effects=True, vmem_limit_bytes=VMEM),
        )(dy, pre, w_down, w_in)
        out = pl.pallas_call(
            kernel_b,
            name="reduce_dx",
            out_shape=[
                arr(SH, D), arr(D, FL), arr(FL, D), arr(D, D),
                arr(8, PR, D), arr(8, PR, D), arr(8, PR, D),
                arr(4, QR, D), arr(4, QR, D), arr(4, QR, D), arr(4, QR, D), arr(4, QR, D),
                arr(PR, D), arr(PR, D),
            ],
            in_specs=[any_] * 7,
            out_specs=[any_] * 14,
            scratch_shapes=[
                pltpu.VMEM((D, FL), BF16), pltpu.VMEM((D, FL), BF16), pltpu.VMEM((D, FL), BF16),
                pltpu.VMEM((D, FL), F32), pltpu.VMEM((QR, D), F32), pltpu.VMEM((2 * SH, D), BF16),
                pltpu.VMEM((2 * SH, FL), BF16), pltpu.VMEM((QR, FL), BF16), pltpu.VMEM((QR, FL), BF16),
                pltpu.VMEM((QR, D), BF16), pltpu.VMEM((QR, D), BF16), pltpu.VMEM((D, 512), BF16), pltpu.VMEM((FL, 512), BF16),
                *gather_sems,
                dma((8,)), dma((8,)), dma((8,)), dma((4,)), dma((4,)), dma((4,)), dma((4,)), dma((4,)), dma((2,)), dma((7,)),
            ],
            compiler_params=pltpu.CompilerParams(collective_id=1, has_side_effects=True, vmem_limit_bytes=VMEM),
        )(x, full, hidden, dpre, dps, w_in, wis)
        return out[0], out[1], out[2]

    rows = P(("dp", "tp"), None)
    cols = P("dp", "tp")
    return jax.shard_map(
        step, mesh=mesh,
        in_specs=(rows, rows, cols, P(None, "tp"), P("tp", None)),
        out_specs=(rows, cols, rows),
        check_vma=False,
    )
```

```python
import functools

import jax
import jax.numpy as jnp
import numpy as np
from jax import lax
from jax.experimental import pallas as pl
from jax.experimental.pallas import tpu as pltpu
from jax.sharding import PartitionSpec as P

MESH = pl.DeviceIdType.MESH
F32, BF16 = jnp.float32, jnp.bfloat16
D = 4096
FL = 1024
SH = 256
CHUNKS_A = ((0, 128, "q"), (128, 128, "q"))
CHUNKS_B = ((0, 112, "p"), (112, 80, "q"), (192, 64, "q"))
PR = 80
QR = 176
VMEM = 66_000_000
NT = (((1,), (1,)), ((), ()))
TN = (((0,), (0,)), ((), ()))


def dot(a, b, dims):
    return lax.dot_general(a, b, dims, preferred_element_type=F32)


def where_am_i():
    tp = lax.axis_index("tp")
    return tp // 8, (tp // 2) % 4, tp % 2


def tp_of(y, z, c):
    return y * 8 + z * 2 + c


def rdma(src, dst, ssem, rsem, dev):
    return pltpu.make_async_remote_copy(
        src_ref=src, dst_ref=dst, send_sem=ssem, recv_sem=rsem, device_id={"tp": dev}, device_id_type=MESH
    )


def greet(y, z, c):
    bar = pltpu.get_barrier_semaphore()

    def hello(dev):
        pl.semaphore_signal(bar, inc=1, device_id={"tp": dev}, device_id_type=MESH)

    hello(tp_of(y, z, 1 - c))
    hello(tp_of(1 - y, z, c))

    @pl.when(z > 0)
    def _():
        hello(tp_of(y, z - 1, c))

    @pl.when(z < 3)
    def _():
        hello(tp_of(y, z + 1, c))

    pl.semaphore_wait(bar, 2 + (z + 2) // 3 + (5 - z) // 3)


class Sends:
    def __init__(self):
        self.all = []

    def start(self, pred, make):
        self.all.append((pred, make))
        if pred is None:
            make().start()
        else:
            pl.when(pred)(lambda: make().start())

    def finish(self):
        for pred, make in self.all:
            if pred is None:
                make().wait_send()
            else:
                pl.when(pred)(lambda make=make: make().wait_send())


class Gather:
    def __init__(self, pos, own, full, rsem, zsem, ysem, sib_s, sib_r, chunks):
        self.y, self.z, self.c = pos
        self.own, self.full = own, full
        self.rsem, self.zsem, self.ysem, self.sib_s, self.sib_r = rsem, zsem, ysem, sib_s, sib_r
        self.chunks = chunks
        self.sends = Sends()

    def rows(self, y, z, k, c=None):
        r0, n = (0, SH) if k is None else self.chunks[k][:2]
        off = tp_of(y, z, self.c if c is None else c) * SH + r0
        return self.full.at[pl.ds(pl.multiple_of(off, 16), n)]

    def copy(self, dev, y, z, k, sems, own):
        r0, n, _ = self.chunks[k]
        src = self.own.at[pl.ds(r0, n)] if own else self.rows(y, z, k)
        d = y * 4 + z
        return rdma(src, self.rows(y, z, k), sems.at[d, k], self.rsem.at[d, k], dev)

    def send_z(self, step, y, z, k, pred=None, own=False):
        ok = self.z > 0 if step < 0 else self.z < 3
        if pred is not None:
            ok = jnp.logical_and(ok, pred)
        dev = tp_of(self.y, self.z + step, self.c)
        self.sends.start(ok, lambda: self.copy(dev, y, z, k, self.zsem.at[(step + 1) // 2], own))

    def send_y(self, y, z, k, pred=None, own=False):
        dev = tp_of(1 - self.y, self.z, self.c)
        self.sends.start(pred, lambda: self.copy(dev, y, z, k, self.ysem, own))

    def wait(self, y, z, k):
        self.copy(tp_of(1 - self.y, self.z, self.c), y, z, k, self.ysem, False).wait_recv()

    def sib_copy(self, y, z, c, own=False):
        d = y * 4 + z
        src = self.own if own else self.rows(y, z, None, c)
        return rdma(src, self.rows(y, z, None, c), self.sib_s.at[d], self.sib_r.at[d], tp_of(self.y, self.z, 1 - self.c))

    def send_sib(self, y, z, pred=None, own=False):
        self.sends.start(pred, lambda: self.sib_copy(y, z, self.c, own))

    def wait_sib(self, y, z):
        self.sib_copy(y, z, 1 - self.c).wait_recv()

    def begin_y(self):
        for k in range(len(self.chunks)):
            self.send_y(self.y, self.z, k, own=True)
        self.send_sib(self.y, self.z, own=True)

    def begin_z(self):
        for k in range(len(self.chunks)):
            self.send_z(1, self.y, self.z, k, own=True)
            self.send_z(-1, self.y, self.z, k, own=True)

    def turn(self):
        y, z = self.y, self.z
        for k, (_, _, kind) in enumerate(self.chunks):
            if kind == "p":
                self.wait(1 - y, z, k)
                self.send_z(1, 1 - y, z, k)
                self.send_z(-1, 1 - y, z, k)

    def step(self, s):
        y, z = self.y, self.z
        for k, (_, _, kind) in enumerate(self.chunks):
            for side in (-1, 1):
                zs = z + side * (s + 1)
                ok = zs >= 0 if side < 0 else zs <= 3
                for ys in (y, 1 - y) if kind == "p" else (y,):
                    pl.when(ok)(lambda ys=ys, zs=zs, k=k: self.wait(ys, zs, k))
                    if s < 2:
                        self.send_z(-side, ys, zs, k, pred=ok)
                if kind == "q":
                    self.send_y(y, zs, k, pred=ok)
        for side in (-1, 1):
            zs = z + side * (s + 1)
            self.send_sib(y, zs, pred=zs >= 0 if side < 0 else zs <= 3)

    def across(self, s):
        y, z = self.y, self.z
        for side in (-1, 1) if s else (0,):
            zs = z + side * s
            ok = None if s == 0 else zs >= 0 if side < 0 else zs <= 3

            def take(zs=zs):
                for k, (_, _, kind) in enumerate(self.chunks):
                    if kind == "q":
                        self.wait(1 - y, zs, k)

            if ok is None:
                take()
            else:
                pl.when(ok)(take)
            self.send_sib(1 - y, zs, pred=ok)


def local(src, dst, sem):
    return pltpu.make_async_copy(src, dst, sem)


def both(*copies):
    for cp in copies:
        cp.start()
    for cp in copies:
        cp.wait()


def kernel(x, dy, pre, w_in, w_down,
           dx, acc_o, dw_down, fy, fx, hidden, dpre, dps, wis, pl_b, pr_b, ps_b, ql_b, qr_b, qs_b, qy_b, qys_b, py_b, pys_b,
           wd_v, wo_v, ws_v, acc, big, blk, a1, a2, arr, obuf, pre_v, hid_v, dp_v,
           y_rs, y_zs, y_ys, y_ss, y_sr, x_rs, x_zs, x_ys, x_ss, x_sr,
           dps_s, dps_r, wis_sem, p_s, pl_r, pr_r, q_s, ql_r, qr_r, qy_s, qy_r, py_sem, lsem):
    y, z, c = where_am_i()
    greet(y, z, c)
    gy = Gather((y, z, c), dy, fy, y_rs, y_zs, y_ys, y_ss, y_sr, CHUNKS_A)
    gx = Gather((y, z, c), x, fx, x_rs, x_zs, x_ys, x_ss, x_sr, CHUNKS_B)
    gy.begin_y()
    gy.begin_z()
    other = tp_of(y, z, 1 - c)
    left, right, over = tp_of(y, z - 1, c), tp_of(y, z + 1, c), tp_of(1 - y, z, c)
    w_copy = rdma(w_in, wis, wis_sem.at[0], wis_sem.at[1], other)
    w_copy.start()
    load_w = local(w_down, wd_v, lsem.at[4])
    load_wo = local(w_in, wo_v, lsem.at[5])
    load_ws = local(wis, ws_v, lsem.at[6])
    load_w.start()
    load_wo.start()
    xv = big.at[pl.ds(0, 2 * SH)]

    def place_own(src, g):
        via = big.at[pl.ds(0, SH)]
        both(local(src, via, lsem.at[0]))
        both(local(via, g.rows(y, z, None), lsem.at[0]))

    def clear():
        def zero(m, _):
            acc[m // 4, pl.ds(pl.multiple_of((m % 4) * 256, 256), 256), :] = jnp.zeros((256, FL), F32)
            return 0

        lax.fori_loop(0, 16, zero, 0)

    def dps_copy(ys, zs):
        off = pl.multiple_of(tp_of(ys, zs, 1 - c) * SH, SH)
        d = ys * 4 + zs
        return rdma(dpre.at[pl.ds(off, SH)], dps.at[pl.ds(pl.multiple_of(d * SH, SH), SH)], dps_s.at[d], dps_r.at[d], other)


    def weigh():
        def weight(j, _):
            ms = pl.ds(pl.multiple_of((j % 4) * 256, 256), 256)
            cols = pl.ds(pl.multiple_of((j // 4) * FL, FL), FL)
            acc[j // 4, ms, :] += dot(hid_v[:, ms], big[0:512, cols], TN)
            return 0

        lax.fori_loop(0, 16, weight, 0)

    def chip_rows(ys, zs):
        return pl.ds(pl.multiple_of(tp_of(ys, zs, 0) * SH, SH), 2 * SH)

    def pair(ys, zs, pred=None, now=True):
        def go():
            gy.wait_sib(ys, zs)
            rows = chip_rows(ys, zs)
            both(local(fy.at[rows], xv, lsem.at[0]), local(pre.at[rows], pre_v, lsem.at[1]))

            def tile(j, _):
                cols = pl.ds(pl.multiple_of(j * 256, 256), 256)
                dh = dot(big[0:512, :], wd_v[cols, :], NT)
                p = pre_v[:, cols].astype(F32)
                k = np.float32(np.sqrt(2 / np.pi))
                t = jnp.tanh(k * (p + 0.044715 * (p * p * p)))
                cdf = 0.5 * (1.0 + t)
                slope = cdf + 0.5 * p * (1.0 - t * t) * (k * (1.0 + 3 * 0.044715 * (p * p)))
                hid_v[:, cols] = (p * cdf).astype(BF16)
                dp_v[:, cols] = (dh * slope).astype(BF16)
                return 0

            lax.fori_loop(0, FL // 256, tile, 0)
            out = local(dp_v, dpre.at[rows], lsem.at[3])
            if now:
                out.start()
                weigh()
                out.wait()
            else:
                both(out, local(hid_v, hidden.at[rows], lsem.at[2]))
            dps_copy(ys, zs).start()

        if pred is None:
            go()
        else:
            pl.when(pred)(go)

    def early(ys, zs, pred):
        pair(ys, zs, pred, now=False)

    def late(ys, zs):
        rows = chip_rows(ys, zs)
        both(local(fy.at[rows], xv, lsem.at[0]), local(hidden.at[rows], hid_v, lsem.at[1]))
        weigh()

    def pairs(do, s, flip):
        def one(i, _):
            zs = z + (2 * i - 1) * s
            do(1 - y if flip else y, zs, jnp.logical_and(zs >= 0, zs <= 3))
            return 0

        lax.fori_loop(0, 2, one, 0)

    place_own(dy, gy)
    clear()
    load_w.wait()
    gy.turn()
    pair(y, z)
    gy.step(0)
    gy.across(0)
    pair(1 - y, z)
    pairs(pair, 1, False)
    gy.step(1)
    gx.begin_z()
    gy.across(1)
    pairs(early, 1, True)
    gy.step(2)
    gx.begin_y()
    pairs(early, 2, False)
    gy.across(2)
    pairs(early, 2, True)
    pairs(early, 3, False)
    w_copy.wait()
    load_ws.start()
    gy.across(3)
    pairs(early, 3, True)


    inner = jnp.logical_and(z > 0, z < 3)
    outer = jnp.logical_not(inner)
    high = z // 2
    inward = 1 - 2 * high
    far = high * z + (1 - high) * (3 - z)

    def target(i):
        o = (0, 1, 5 - far, far)[i]
        return high * o + (1 - high) * (3 - o)

    def fetch(ys, zs, r0, n, at):
        o = pl.multiple_of(tp_of(ys, zs, c) * SH + r0, 16)
        s = pl.multiple_of((ys * 4 + zs) * SH + r0, 16)
        return (local(dpre.at[pl.ds(o, n)], a1.at[pl.ds(at, n)], lsem.at[0]),
                local(dps.at[pl.ds(s, n)], a2.at[pl.ds(at, n)], lsem.at[1]))

    def fetch_all(parts):
        for part in parts:
            both(*part)

    def cols512(j):
        return pl.ds(pl.multiple_of(j * 512, 512), 512)

    def q_terms():
        fetch_all([fetch(1 - y, target(i), PR, QR, i * QR) for i in range(4)])

        def tile(j, _):
            cols = cols512(j)
            big[:, cols] = (dot(a1[...], wo_v[cols, :], NT) + dot(a2[...], ws_v[cols, :], NT)).astype(BF16)
            return 0

        lax.fori_loop(0, D // 512, tile, 0)
        both(*(local(big.at[pl.ds(i * QR, QR)], qys_b.at[target(i)], lsem.at[i]) for i in range(4)))

    def terms(v):
        fetch_all([fetch(1 - y, v, 0, PR, 0), fetch(y, v, 0, SH, PR)])
        n = PR + SH

        def tile(j, _):
            cols = cols512(j)
            blk[:, cols] = dot(a1[0:n, :], wo_v[cols, :], NT) + dot(a2[0:n, :], ws_v[cols, :], NT)
            return 0

        lax.fori_loop(0, D // 512, tile, 0)

    def add(buf, copy, at, n):
        copy.wait_recv()
        both(local(buf, arr.at[pl.ds(0, n)], lsem.at[2]))

        def tile(j, _):
            cols = cols512(j)
            blk[at:at + n, cols] += arr[0:n, cols].astype(F32)
            return 0

        lax.fori_loop(0, D // 512, tile, 0)

    def store(buf, at, n):
        def tile(j, _):
            cols = cols512(j)
            obuf[0:n, cols] = blk[at:at + n, cols].astype(BF16)
            return 0

        lax.fori_loop(0, D // 512, tile, 0)
        both(local(obuf.at[pl.ds(0, n)], buf, lsem.at[3]))

    def p_copy(ys, v, dev, rightward):
        i = ys * 4 + v
        dst, sem = (pl_b, pl_r) if rightward else (pr_b, pr_r)
        return rdma(ps_b.at[i], dst.at[i], p_s.at[i], sem.at[i], dev)

    def q_copy(v, dev, rightward):
        dst, sem = (ql_b, ql_r) if rightward else (qr_b, qr_r)
        return rdma(qs_b.at[v], dst.at[v], q_s.at[v], sem.at[v], dev)

    def qy_copy(v):
        return rdma(qys_b.at[v], qy_b.at[v], qy_s.at[v], qy_r.at[v], over)

    def py_copy():
        return rdma(pys_b, py_b, py_sem.at[0], py_sem.at[1], over)

    def from_left(ok, ys, v, at):
        if ys is None:
            pl.when(ok)(lambda: add(ql_b.at[v], q_copy(v, right, True), at, QR))
        else:
            pl.when(ok)(lambda: add(pl_b.at[ys * 4 + v], p_copy(ys, v, right, True), at, PR))

    def from_right(ok, ys, v, at):
        if ys is None:
            pl.when(ok)(lambda: add(qr_b.at[v], q_copy(v, left, False), at, QR))
        else:
            pl.when(ok)(lambda: add(pr_b.at[ys * 4 + v], p_copy(ys, v, left, False), at, PR))

    def towards(i, pred, fill=(None, None)):
        v = target(i)
        up, down = v > z, v < z

        def go():
            terms(v)
            for ys, at, other_work in ((1 - y, 0, fill[0]), (y, PR, fill[1])):
                from_left(jnp.logical_and(inner, up), ys, v, at)
                from_right(jnp.logical_and(inner, down), ys, v, at)
                store(ps_b.at[ys * 4 + v], at, PR)
                pl.when(up)(lambda ys=ys: p_copy(ys, v, right, True).start())
                pl.when(down)(lambda ys=ys: p_copy(ys, v, left, False).start())
                if other_work is not None:
                    other_work()
            add(qy_b.at[v], qy_copy(v), 2 * PR, QR)
            from_left(jnp.logical_and(inner, up), None, v, 2 * PR)
            from_right(jnp.logical_and(inner, down), None, v, 2 * PR)
            store(qs_b.at[v], 2 * PR, QR)
            pl.when(up)(lambda: q_copy(v, right, True).start())
            pl.when(down)(lambda: q_copy(v, left, False).start())

        pl.when(pred)(go)

    def arrived(ys, at):
        from_left(z > 0, ys, z, at)
        from_right(z < 3, ys, z, at)

    def in_step(ys, zs, pred=None):
        def go():
            gx.wait_sib(ys, zs)
            rows = chip_rows(ys, zs)
            both(local(fx.at[rows], xv, lsem.at[0]), local(dpre.at[rows], dp_v, lsem.at[1]))

            def row(m, _):
                here = pl.ds(pl.multiple_of((m % 4) * 256, 256), 256)
                acc[m // 4, here, :] += dot(big[0:512, pl.ds(pl.multiple_of(m * 256, 256), 256)], dp_v[...], TN)
                return 0

            lax.fori_loop(0, D // 256, row, 0)

        if pred is None:
            go()
        else:
            pl.when(pred)(go)

    def write(to):
        def one(m, _):
            h0, h1 = pl.ds(0, 512), pl.ds(512, 512)
            hid_v[...] = acc[m, h0, :].astype(BF16)
            first = local(hid_v, to(m, 0), lsem.at[0])
            first.start()
            pre_v[...] = acc[m, h1, :].astype(BF16)
            both(local(pre_v, to(m, 1), lsem.at[1]))
            first.wait()
            return 0

        lax.fori_loop(0, 4, one, 0)

    for d in range(8):
        cp = rdma(dpre.at[pl.ds(0, SH)], dps.at[pl.ds(d * SH, SH)], dps_s.at[d], dps_r.at[d], other)
        cp.wait_recv()
        cp.wait_send()
    load_wo.wait()
    load_ws.wait()
    q_terms()
    qy_copy(target(0)).start()
    qy_copy(target(1)).start()
    gx.turn()
    place_own(x, gx)
    towards(0, outer)

    def late_first(k, _):
        late(jnp.where(inner, 1 - y, jnp.where(k == 0, 1 - y, y)), z + inward * jnp.where(inner, 1 - 2 * k, 1 + k))
        return 0

    def late_rest(k, _):
        late(jnp.where(k % 2 == 0, 1 - y, y), z + inward * (1 + (k + 1) // 2))
        return 0

    lax.fori_loop(0, 2, late_first, 0)
    gx.step(0)
    gx.across(0)
    qy_copy(target(2)).start()
    towards(0, inner, (lambda: late(y, z + 2 * inward), lambda: late(1 - y, z + 2 * inward)))
    towards(1, outer)
    gx.step(1)
    qy_copy(target(3)).start()
    lax.fori_loop(2, jnp.where(inner, 2, 5), late_rest, 0)
    write(lambda m, h: dw_down.at[pl.ds(h * 512, 512), pl.ds(pl.multiple_of(m * FL, FL), FL)])
    clear()
    in_step(y, z)
    in_step(1 - y, z, outer)
    towards(1, inner, (lambda: in_step(1 - y, z), lambda: in_step(y, z - 1)))
    towards(2, outer)
    gx.across(1)
    gx.step(2)
    towards(2, inner)
    in_step(y, jnp.where(inner, z + 1, z + inward))
    pairs(in_step, 1, True)
    gx.across(2)
    in_step(y, z + 2 * inward, outer)
    in_step(1 - y, z + 2 * inward, outer)
    save = local(acc, acc_o, lsem.at[4])
    save.start()
    terms(z)
    arrived(1 - y, 0)
    store(pys_b, 0, PR)
    py_copy().start()
    add(qy_b.at[z], qy_copy(z), 2 * PR, QR)
    arrived(None, 2 * PR)
    store(dx.at[pl.ds(PR, QR)], 2 * PR, QR)
    arrived(y, PR)
    add(py_b, py_copy(), PR, PR)
    store(dx.at[pl.ds(0, PR)], PR, PR)
    gx.across(3)
    gx.wait_sib(y, 3 - 3 * high)
    gx.wait_sib(1 - y, 3 - 3 * high)
    save.wait()

    for i in range(3):
        v = target(i)
        for ys in (1 - y, y):
            p_copy(ys, v, left, False).wait_send()
        q_copy(v, left, False).wait_send()
    for i in range(4):
        qy_copy(target(i)).wait_send()
    py_copy().wait_send()
    gy.sends.finish()
    gx.sends.finish()


def place(acc, x0, x1, dp0, dp1, down_in, dx_in, dw_in, down, dx):
    total = acc[...] + dot(x0[...], dp0[...], TN) + dot(x1[...], dp1[...], TN)
    dw_in[...] = total.astype(BF16)
    down[...] = down_in[...]
    dx[...] = dx_in[...]


def finish(acc, full, dpre, down, dx):
    def chip(other):
        tp = lax.axis_index("tp")
        y = tp // 8
        return (1 - y if other else y) * 4 + 3 - 3 * ((tp // 2) % 4 // 2)

    steps = 8
    tall = pl.BlockSpec((FL // steps, D), lambda i: (i, 0))
    flat = pl.BlockSpec((SH // steps, D), lambda i: (i, 0))
    part = pl.BlockSpec((D // steps, FL), lambda i: (i, 0))
    return pl.pallas_call(
        place,
        name="finish",
        grid=(steps,),
        in_specs=[
            part,
            pl.BlockSpec((2 * SH, D // steps), lambda i: (chip(False), i)),
            pl.BlockSpec((2 * SH, D // steps), lambda i: (chip(True), i)),
            pl.BlockSpec((2 * SH, FL), lambda i: (chip(False), 0)),
            pl.BlockSpec((2 * SH, FL), lambda i: (chip(True), 0)),
            tall, flat,
        ],
        out_specs=[part, tall, flat],
        out_shape=[jax.ShapeDtypeStruct(s, BF16) for s in ((D, FL), (FL, D), (SH, D))],
        compiler_params=pltpu.CompilerParams(vmem_limit_bytes=48_000_000),
    )(acc.reshape(D, FL), full, full, dpre, dpre, down, dx)


def solution(mesh):
    any_ = pl.BlockSpec(memory_space=pl.ANY)
    dma = pltpu.SemaphoreType.DMA

    def arr(*shape):
        return jax.ShapeDtypeStruct(shape, BF16)

    def vmem(*shape, dtype=BF16):
        return pltpu.VMEM(shape, dtype)

    gather_sems = [dma((8, 3)), dma((2, 8, 3)), dma((8, 3)), dma((8,)), dma((8,))]

    def step(x, dy, pre, w_in, w_down):
        outs = [
            arr(SH, D), jax.ShapeDtypeStruct((4, FL, FL), F32), arr(FL, D), arr(D, D), arr(D, D),
            arr(D, FL), arr(D, FL), arr(8 * SH, FL), arr(D, FL),
            arr(8, PR, D), arr(8, PR, D), arr(8, PR, D),
            arr(4, QR, D), arr(4, QR, D), arr(4, QR, D), arr(4, QR, D), arr(4, QR, D),
            arr(PR, D), arr(PR, D),
        ]
        out = pl.pallas_call(
            kernel,
            name="backward",
            out_shape=outs,
            in_specs=[any_] * 5,
            out_specs=[any_] * len(outs),
            scratch_shapes=[
                vmem(FL, D), vmem(D, FL), vmem(D, FL), vmem(4, FL, FL, dtype=F32), vmem(4 * QR, D),
                vmem(PR + SH, D, dtype=F32), vmem(4 * QR, FL), vmem(4 * QR, FL), vmem(QR, D), vmem(QR, D),
                vmem(2 * SH, FL), vmem(2 * SH, FL), vmem(2 * SH, FL),
                *gather_sems, *gather_sems, dma((8,)), dma((8,)), dma((2,)),
                dma((8,)), dma((8,)), dma((8,)), dma((4,)), dma((4,)), dma((4,)), dma((4,)), dma((4,)), dma((2,)), dma((7,)),
            ],
            compiler_params=pltpu.CompilerParams(collective_id=0, has_side_effects=True, vmem_limit_bytes=VMEM),
        )(x, dy, pre, w_in, w_down)
        dx, acc, down, _, full, _, dpre = out[:7]
        dw_in, dw_down, dx = finish(acc, full, dpre, down, dx)
        return dx, dw_in, dw_down

    rows = P(("dp", "tp"), None)
    cols = P("dp", "tp")
    return jax.shard_map(
        step, mesh=mesh,
        in_specs=(rows, rows, cols, P(None, "tp"), P("tp", None)),
        out_specs=(rows, cols, rows),
        check_vma=False,
    )
```

```python
import functools

import jax
import jax.numpy as jnp
import numpy as np
from jax import lax
from jax.experimental import pallas as pl
from jax.experimental.pallas import tpu as pltpu
from jax.sharding import PartitionSpec as P

MESH = pl.DeviceIdType.MESH
F32, BF16 = jnp.float32, jnp.bfloat16
D = 4096
FL = 1024
SH = 256
CHUNKS_A = ((0, 16, "p"), (16, 80, "q"), (96, 80, "q"), (176, 80, "q"))
CHUNKS_B = ((0, 128, "p"), (128, 64, "q"), (192, 64, "q"))
PR = 80
QR = 176
VMEM = 66_000_000
NT = (((1,), (1,)), ((), ()))
TN = (((0,), (0,)), ((), ()))


def dot(a, b, dims):
    return lax.dot_general(a, b, dims, preferred_element_type=F32)


def where_am_i():
    tp = lax.axis_index("tp")
    return tp // 8, (tp // 2) % 4, tp % 2


def tp_of(y, z, c):
    return y * 8 + z * 2 + c


def rdma(src, dst, ssem, rsem, dev):
    return pltpu.make_async_remote_copy(
        src_ref=src, dst_ref=dst, send_sem=ssem, recv_sem=rsem, device_id={"tp": dev}, device_id_type=MESH
    )


def greet(y, z, c):
    bar = pltpu.get_barrier_semaphore()

    def hello(dev):
        pl.semaphore_signal(bar, inc=1, device_id={"tp": dev}, device_id_type=MESH)

    hello(tp_of(y, z, 1 - c))
    hello(tp_of(1 - y, z, c))

    @pl.when(z > 0)
    def _():
        hello(tp_of(y, z - 1, c))

    @pl.when(z < 3)
    def _():
        hello(tp_of(y, z + 1, c))

    pl.semaphore_wait(bar, 2 + (z + 2) // 3 + (5 - z) // 3)


class Sends:
    def __init__(self):
        self.all = []

    def start(self, pred, make):
        self.all.append((pred, make))
        if pred is None:
            make().start()
        else:
            pl.when(pred)(lambda: make().start())

    def finish(self):
        for pred, make in self.all:
            if pred is None:
                make().wait_send()
            else:
                pl.when(pred)(lambda make=make: make().wait_send())


class Gather:
    def __init__(self, pos, own, full, rsem, zsem, ysem, sib_s, sib_r, chunks):
        self.y, self.z, self.c = pos
        self.own, self.full = own, full
        self.rsem, self.zsem, self.ysem, self.sib_s, self.sib_r = rsem, zsem, ysem, sib_s, sib_r
        self.chunks = chunks
        self.sends = Sends()

    def rows(self, y, z, k, c=None):
        r0, n = (0, SH) if k is None else self.chunks[k][:2]
        off = tp_of(y, z, self.c if c is None else c) * SH + r0
        return self.full.at[pl.ds(pl.multiple_of(off, 16), n)]

    def copy(self, dev, y, z, k, sems, own):
        r0, n, _ = self.chunks[k]
        src = self.own.at[pl.ds(r0, n)] if own else self.rows(y, z, k)
        d = y * 4 + z
        return rdma(src, self.rows(y, z, k), sems.at[d, k], self.rsem.at[d, k], dev)

    def send_z(self, step, y, z, k, pred=None, own=False):
        ok = self.z > 0 if step < 0 else self.z < 3
        if pred is not None:
            ok = jnp.logical_and(ok, pred)
        dev = tp_of(self.y, self.z + step, self.c)
        self.sends.start(ok, lambda: self.copy(dev, y, z, k, self.zsem.at[(step + 1) // 2], own))

    def send_y(self, y, z, k, pred=None, own=False):
        dev = tp_of(1 - self.y, self.z, self.c)
        self.sends.start(pred, lambda: self.copy(dev, y, z, k, self.ysem, own))

    def wait(self, y, z, k):
        self.copy(tp_of(1 - self.y, self.z, self.c), y, z, k, self.ysem, False).wait_recv()

    def sib_copy(self, y, z, c, own=False):
        d = y * 4 + z
        src = self.own if own else self.rows(y, z, None, c)
        return rdma(src, self.rows(y, z, None, c), self.sib_s.at[d], self.sib_r.at[d], tp_of(self.y, self.z, 1 - self.c))

    def send_sib(self, y, z, pred=None, own=False):
        self.sends.start(pred, lambda: self.sib_copy(y, z, self.c, own))

    def wait_sib(self, y, z):
        self.sib_copy(y, z, 1 - self.c).wait_recv()

    def begin_y(self):
        for k in range(len(self.chunks)):
            self.send_y(self.y, self.z, k, own=True)
        self.send_sib(self.y, self.z, own=True)

    def begin_z(self):
        for k in range(len(self.chunks)):
            self.send_z(1, self.y, self.z, k, own=True)
            self.send_z(-1, self.y, self.z, k, own=True)

    def turn(self):
        y, z = self.y, self.z
        for k, (_, _, kind) in enumerate(self.chunks):
            if kind == "p":
                self.wait(1 - y, z, k)
                self.send_z(1, 1 - y, z, k)
                self.send_z(-1, 1 - y, z, k)

    def step(self, s):
        y, z = self.y, self.z
        for k, (_, _, kind) in enumerate(self.chunks):
            for side in (-1, 1):
                zs = z + side * (s + 1)
                ok = zs >= 0 if side < 0 else zs <= 3
                for ys in (y, 1 - y) if kind == "p" else (y,):
                    pl.when(ok)(lambda ys=ys, zs=zs, k=k: self.wait(ys, zs, k))
                    if s < 2:
                        self.send_z(-side, ys, zs, k, pred=ok)
                if kind == "q":
                    self.send_y(y, zs, k, pred=ok)
        for side in (-1, 1):
            zs = z + side * (s + 1)
            self.send_sib(y, zs, pred=zs >= 0 if side < 0 else zs <= 3)

    def across(self, s):
        y, z = self.y, self.z
        for side in (-1, 1) if s else (0,):
            zs = z + side * s
            ok = None if s == 0 else zs >= 0 if side < 0 else zs <= 3

            def take(zs=zs):
                for k, (_, _, kind) in enumerate(self.chunks):
                    if kind == "q":
                        self.wait(1 - y, zs, k)

            if ok is None:
                take()
            else:
                pl.when(ok)(take)
            self.send_sib(1 - y, zs, pred=ok)


def local(src, dst, sem):
    return pltpu.make_async_copy(src, dst, sem)


def both(*copies):
    for cp in copies:
        cp.start()
    for cp in copies:
        cp.wait()


def kernel(x, dy, pre, w_in, w_down,
           dx, acc_o, dw_down, fy, fx, hidden, dpre, dps, wis, pl_b, pr_b, ps_b, ql_b, qr_b, qs_b, qy_b, qys_b, py_b, pys_b,
           wd_v, wo_v, ws_v, acc, big, blk, a1, a2, arr, obuf, pre_v, hid_v, dp_v,
           y_rs, y_zs, y_ys, y_ss, y_sr, x_rs, x_zs, x_ys, x_ss, x_sr,
           dps_s, dps_r, wis_sem, p_s, pl_r, pr_r, q_s, ql_r, qr_r, qy_s, qy_r, py_sem, lsem):
    y, z, c = where_am_i()
    greet(y, z, c)
    gy = Gather((y, z, c), dy, fy, y_rs, y_zs, y_ys, y_ss, y_sr, CHUNKS_A)
    gx = Gather((y, z, c), x, fx, x_rs, x_zs, x_ys, x_ss, x_sr, CHUNKS_B)
    gy.begin_y()
    gy.begin_z()
    other = tp_of(y, z, 1 - c)
    left, right, over = tp_of(y, z - 1, c), tp_of(y, z + 1, c), tp_of(1 - y, z, c)
    w_copy = rdma(w_in, wis, wis_sem.at[0], wis_sem.at[1], other)
    w_copy.start()
    load_w = local(w_down, wd_v, lsem.at[4])
    load_wo = local(w_in, wo_v, lsem.at[5])
    load_ws = local(wis, ws_v, lsem.at[6])
    load_w.start()
    load_wo.start()
    xv = big.at[pl.ds(0, 2 * SH)]

    def place_own(src, g):
        via = big.at[pl.ds(0, SH)]
        both(local(src, via, lsem.at[0]))
        both(local(via, g.rows(y, z, None), lsem.at[0]))

    def clear():
        def zero(m, _):
            acc[m // 4, pl.ds(pl.multiple_of((m % 4) * 256, 256), 256), :] = jnp.zeros((256, FL), F32)
            return 0

        lax.fori_loop(0, 16, zero, 0)

    def dps_copy(ys, zs):
        off = pl.multiple_of(tp_of(ys, zs, 1 - c) * SH, SH)
        d = ys * 4 + zs
        return rdma(dpre.at[pl.ds(off, SH)], dps.at[pl.ds(pl.multiple_of(d * SH, SH), SH)], dps_s.at[d], dps_r.at[d], other)


    def weigh():
        def weight(j, _):
            ms = pl.ds(pl.multiple_of((j % 4) * 256, 256), 256)
            cols = pl.ds(pl.multiple_of((j // 4) * FL, FL), FL)
            acc[j // 4, ms, :] += dot(hid_v[:, ms], big[0:512, cols], TN)
            return 0

        lax.fori_loop(0, 16, weight, 0)

    def chip_rows(ys, zs):
        return pl.ds(pl.multiple_of(tp_of(ys, zs, 0) * SH, SH), 2 * SH)

    def pair(ys, zs, pred=None, now=True):
        def go():
            gy.wait_sib(ys, zs)
            rows = chip_rows(ys, zs)
            both(local(fy.at[rows], xv, lsem.at[0]), local(pre.at[rows], pre_v, lsem.at[1]))

            def tile(j, _):
                cols = pl.ds(pl.multiple_of(j * 256, 256), 256)
                dh = dot(big[0:512, :], wd_v[cols, :], NT)
                p = pre_v[:, cols].astype(F32)
                k = np.float32(np.sqrt(2 / np.pi))
                t = jnp.tanh(k * (p + 0.044715 * (p * p * p)))
                cdf = 0.5 * (1.0 + t)
                slope = cdf + 0.5 * p * (1.0 - t * t) * (k * (1.0 + 3 * 0.044715 * (p * p)))
                hid_v[:, cols] = (p * cdf).astype(BF16)
                dp_v[:, cols] = (dh * slope).astype(BF16)
                return 0

            lax.fori_loop(0, FL // 256, tile, 0)
            out = local(dp_v, dpre.at[rows], lsem.at[3])
            if now:
                out.start()
                weigh()
                out.wait()
            else:
                both(out, local(hid_v, hidden.at[rows], lsem.at[2]))
            dps_copy(ys, zs).start()

        if pred is None:
            go()
        else:
            pl.when(pred)(go)

    def early(ys, zs, pred):
        pair(ys, zs, pred, now=False)

    def late(ys, zs):
        rows = chip_rows(ys, zs)
        both(local(fy.at[rows], xv, lsem.at[0]), local(hidden.at[rows], hid_v, lsem.at[1]))
        weigh()

    def pairs(do, s, flip):
        def one(i, _):
            zs = z + (2 * i - 1) * s
            do(1 - y if flip else y, zs, jnp.logical_and(zs >= 0, zs <= 3))
            return 0

        lax.fori_loop(0, 2, one, 0)

    place_own(dy, gy)
    clear()
    load_w.wait()
    gy.turn()
    pair(y, z)
    gy.step(0)
    gy.across(0)
    pair(1 - y, z)
    pairs(pair, 1, False)
    gy.step(1)
    gx.begin_z()
    place_own(x, gx)
    gy.across(1)
    pairs(early, 1, True)
    gy.step(2)
    gx.begin_y()
    pairs(early, 2, False)
    gy.across(2)
    pairs(early, 2, True)
    pairs(early, 3, False)
    w_copy.wait()
    load_ws.start()
    gy.across(3)
    pairs(early, 3, True)


    inner = jnp.logical_and(z > 0, z < 3)
    outer = jnp.logical_not(inner)
    high = z // 2
    inward = 1 - 2 * high
    far = high * z + (1 - high) * (3 - z)

    def target(i):
        o = (0, 1, 5 - far, far)[i]
        return high * o + (1 - high) * (3 - o)

    def fetch(ys, zs, r0, n, at):
        o = pl.multiple_of(tp_of(ys, zs, c) * SH + r0, 16)
        s = pl.multiple_of((ys * 4 + zs) * SH + r0, 16)
        return (local(dpre.at[pl.ds(o, n)], a1.at[pl.ds(at, n)], lsem.at[0]),
                local(dps.at[pl.ds(s, n)], a2.at[pl.ds(at, n)], lsem.at[1]))

    def fetch_all(parts):
        for part in parts:
            both(*part)

    def cols512(j):
        return pl.ds(pl.multiple_of(j * 512, 512), 512)

    def q_terms():
        fetch_all([fetch(1 - y, target(i), PR, QR, i * QR) for i in range(4)])

        def tile(j, _):
            cols = cols512(j)
            big[:, cols] = (dot(a1[...], wo_v[cols, :], NT) + dot(a2[...], ws_v[cols, :], NT)).astype(BF16)
            return 0

        lax.fori_loop(0, D // 512, tile, 0)
        both(*(local(big.at[pl.ds(i * QR, QR)], qys_b.at[target(i)], lsem.at[i]) for i in range(4)))

    def terms(v):
        fetch_all([fetch(1 - y, v, 0, PR, 0), fetch(y, v, 0, SH, PR)])
        n = PR + SH

        def tile(j, _):
            cols = cols512(j)
            blk[:, cols] = dot(a1[0:n, :], wo_v[cols, :], NT) + dot(a2[0:n, :], ws_v[cols, :], NT)
            return 0

        lax.fori_loop(0, D // 512, tile, 0)

    def add(buf, copy, at, n):
        copy.wait_recv()
        both(local(buf, arr.at[pl.ds(0, n)], lsem.at[2]))

        def tile(j, _):
            cols = cols512(j)
            blk[at:at + n, cols] += arr[0:n, cols].astype(F32)
            return 0

        lax.fori_loop(0, D // 512, tile, 0)

    def store(buf, at, n):
        def tile(j, _):
            cols = cols512(j)
            obuf[0:n, cols] = blk[at:at + n, cols].astype(BF16)
            return 0

        lax.fori_loop(0, D // 512, tile, 0)
        both(local(obuf.at[pl.ds(0, n)], buf, lsem.at[3]))

    def p_copy(ys, v, dev, rightward):
        i = ys * 4 + v
        dst, sem = (pl_b, pl_r) if rightward else (pr_b, pr_r)
        return rdma(ps_b.at[i], dst.at[i], p_s.at[i], sem.at[i], dev)

    def q_copy(v, dev, rightward):
        dst, sem = (ql_b, ql_r) if rightward else (qr_b, qr_r)
        return rdma(qs_b.at[v], dst.at[v], q_s.at[v], sem.at[v], dev)

    def qy_copy(v):
        return rdma(qys_b.at[v], qy_b.at[v], qy_s.at[v], qy_r.at[v], over)

    def py_copy():
        return rdma(pys_b, py_b, py_sem.at[0], py_sem.at[1], over)

    def from_left(ok, ys, v, at):
        if ys is None:
            pl.when(ok)(lambda: add(ql_b.at[v], q_copy(v, right, True), at, QR))
        else:
            pl.when(ok)(lambda: add(pl_b.at[ys * 4 + v], p_copy(ys, v, right, True), at, PR))

    def from_right(ok, ys, v, at):
        if ys is None:
            pl.when(ok)(lambda: add(qr_b.at[v], q_copy(v, left, False), at, QR))
        else:
            pl.when(ok)(lambda: add(pr_b.at[ys * 4 + v], p_copy(ys, v, left, False), at, PR))

    def towards(i, pred, fill=(None, None)):
        v = target(i)
        up, down = v > z, v < z

        def go():
            terms(v)
            for ys, at, other_work in ((1 - y, 0, fill[0]), (y, PR, fill[1])):
                from_left(jnp.logical_and(inner, up), ys, v, at)
                from_right(jnp.logical_and(inner, down), ys, v, at)
                store(ps_b.at[ys * 4 + v], at, PR)
                pl.when(up)(lambda ys=ys: p_copy(ys, v, right, True).start())
                pl.when(down)(lambda ys=ys: p_copy(ys, v, left, False).start())
                if other_work is not None:
                    other_work()
            add(qy_b.at[v], qy_copy(v), 2 * PR, QR)
            from_left(jnp.logical_and(inner, up), None, v, 2 * PR)
            from_right(jnp.logical_and(inner, down), None, v, 2 * PR)
            store(qs_b.at[v], 2 * PR, QR)
            pl.when(up)(lambda: q_copy(v, right, True).start())
            pl.when(down)(lambda: q_copy(v, left, False).start())

        pl.when(pred)(go)

    def arrived(ys, at):
        from_left(z > 0, ys, z, at)
        from_right(z < 3, ys, z, at)

    def in_step(ys, zs, pred=None):
        def go():
            gx.wait_sib(ys, zs)
            rows = chip_rows(ys, zs)
            both(local(fx.at[rows], xv, lsem.at[0]), local(dpre.at[rows], dp_v, lsem.at[1]))

            def row(m, _):
                here = pl.ds(pl.multiple_of((m % 4) * 256, 256), 256)
                acc[m // 4, here, :] += dot(big[0:512, pl.ds(pl.multiple_of(m * 256, 256), 256)], dp_v[...], TN)
                return 0

            lax.fori_loop(0, D // 256, row, 0)

        if pred is None:
            go()
        else:
            pl.when(pred)(go)

    def write(to):
        def one(m, _):
            h0, h1 = pl.ds(0, 512), pl.ds(512, 512)
            hid_v[...] = acc[m, h0, :].astype(BF16)
            first = local(hid_v, to(m, 0), lsem.at[0])
            first.start()
            pre_v[...] = acc[m, h1, :].astype(BF16)
            both(local(pre_v, to(m, 1), lsem.at[1]))
            first.wait()
            return 0

        lax.fori_loop(0, 4, one, 0)

    for d in range(8):
        cp = rdma(dpre.at[pl.ds(0, SH)], dps.at[pl.ds(d * SH, SH)], dps_s.at[d], dps_r.at[d], other)
        cp.wait_recv()
        cp.wait_send()
    gx.turn()
    load_wo.wait()
    load_ws.wait()
    q_terms()
    qy_copy(target(0)).start()
    qy_copy(target(1)).start()
    towards(0, outer)
    gx.step(0)

    def late_first(k, _):
        late(jnp.where(inner, 1 - y, jnp.where(k == 0, 1 - y, y)), z + inward * jnp.where(inner, 1 - 2 * k, 1 + k))
        return 0

    def late_rest(k, _):
        late(jnp.where(k % 2 == 0, 1 - y, y), z + inward * (1 + (k + 1) // 2))
        return 0

    lax.fori_loop(0, 2, late_first, 0)
    gx.across(0)
    qy_copy(target(2)).start()
    towards(0, inner, (lambda: late(y, z + 2 * inward), lambda: late(1 - y, z + 2 * inward)))
    towards(1, outer)
    gx.step(1)
    qy_copy(target(3)).start()
    lax.fori_loop(2, jnp.where(inner, 2, 5), late_rest, 0)
    write(lambda m, h: dw_down.at[pl.ds(h * 512, 512), pl.ds(pl.multiple_of(m * FL, FL), FL)])
    clear()
    in_step(y, z)
    in_step(1 - y, z, outer)
    towards(1, inner, (lambda: in_step(1 - y, z), lambda: in_step(y, z - 1)))
    towards(2, outer)
    gx.across(1)
    gx.step(2)
    towards(2, inner)

    def pass_over():
        terms(z)
        arrived(1 - y, 0)
        store(pys_b, 0, PR)
        py_copy().start()

    in_step(y, jnp.where(inner, z + 1, z + inward))
    pl.when(inner)(pass_over)
    pairs(in_step, 1, True)
    pl.when(outer)(pass_over)
    gx.across(2)
    in_step(y, z + 2 * inward, outer)
    in_step(1 - y, z + 2 * inward, outer)
    save = local(acc, acc_o, lsem.at[4])
    save.start()
    terms(z)
    add(qy_b.at[z], qy_copy(z), 2 * PR, QR)
    arrived(None, 2 * PR)
    store(dx.at[pl.ds(PR, QR)], 2 * PR, QR)
    arrived(y, PR)
    add(py_b, py_copy(), PR, PR)
    store(dx.at[pl.ds(0, PR)], PR, PR)
    gx.across(3)
    gx.wait_sib(y, 3 - 3 * high)
    gx.wait_sib(1 - y, 3 - 3 * high)
    save.wait()

    for i in range(3):
        v = target(i)
        for ys in (1 - y, y):
            p_copy(ys, v, left, False).wait_send()
        q_copy(v, left, False).wait_send()
    for i in range(4):
        qy_copy(target(i)).wait_send()
    py_copy().wait_send()
    gy.sends.finish()
    gx.sends.finish()


def place(acc, x0, x1, dp0, dp1, down_in, dx_in, dw_in, down, dx):
    total = acc[...] + dot(x0[...], dp0[...], TN) + dot(x1[...], dp1[...], TN)
    dw_in[...] = total.astype(BF16)
    down[...] = down_in[...]
    dx[...] = dx_in[...]


def finish(acc, full, dpre, down, dx):
    def chip(other):
        tp = lax.axis_index("tp")
        y = tp // 8
        return (1 - y if other else y) * 4 + 3 - 3 * ((tp // 2) % 4 // 2)

    steps = 8
    tall = pl.BlockSpec((FL // steps, D), lambda i: (i, 0))
    flat = pl.BlockSpec((SH // steps, D), lambda i: (i, 0))
    part = pl.BlockSpec((D // steps, FL), lambda i: (i, 0))
    return pl.pallas_call(
        place,
        name="finish",
        grid=(steps,),
        in_specs=[
            part,
            pl.BlockSpec((2 * SH, D // steps), lambda i: (chip(False), i)),
            pl.BlockSpec((2 * SH, D // steps), lambda i: (chip(True), i)),
            pl.BlockSpec((2 * SH, FL), lambda i: (chip(False), 0)),
            pl.BlockSpec((2 * SH, FL), lambda i: (chip(True), 0)),
            tall, flat,
        ],
        out_specs=[part, tall, flat],
        out_shape=[jax.ShapeDtypeStruct(s, BF16) for s in ((D, FL), (FL, D), (SH, D))],
        compiler_params=pltpu.CompilerParams(vmem_limit_bytes=VMEM),
    )(acc.reshape(D, FL), full, full, dpre, dpre, down, dx)


def solution(mesh):
    any_ = pl.BlockSpec(memory_space=pl.ANY)
    dma = pltpu.SemaphoreType.DMA

    def arr(*shape):
        return jax.ShapeDtypeStruct(shape, BF16)

    def vmem(*shape, dtype=BF16):
        return pltpu.VMEM(shape, dtype)

    gather_sems = [dma((8, 4)), dma((2, 8, 4)), dma((8, 4)), dma((8,)), dma((8,))]

    def step(x, dy, pre, w_in, w_down):
        outs = [
            arr(SH, D), jax.ShapeDtypeStruct((4, FL, FL), F32), arr(FL, D), arr(D, D), arr(D, D),
            arr(D, FL), arr(D, FL), arr(8 * SH, FL), arr(D, FL),
            arr(8, PR, D), arr(8, PR, D), arr(8, PR, D),
            arr(4, QR, D), arr(4, QR, D), arr(4, QR, D), arr(4, QR, D), arr(4, QR, D),
            arr(PR, D), arr(PR, D),
        ]
        out = pl.pallas_call(
            kernel,
            name="backward",
            out_shape=outs,
            in_specs=[any_] * 5,
            out_specs=[any_] * len(outs),
            scratch_shapes=[
                vmem(FL, D), vmem(D, FL), vmem(D, FL), vmem(4, FL, FL, dtype=F32), vmem(4 * QR, D),
                vmem(PR + SH, D, dtype=F32), vmem(4 * QR, FL), vmem(4 * QR, FL), vmem(QR, D), vmem(QR, D),
                vmem(2 * SH, FL), vmem(2 * SH, FL), vmem(2 * SH, FL),
                *gather_sems, *gather_sems, dma((8,)), dma((8,)), dma((2,)),
                dma((8,)), dma((8,)), dma((8,)), dma((4,)), dma((4,)), dma((4,)), dma((4,)), dma((4,)), dma((2,)), dma((7,)),
            ],
            compiler_params=pltpu.CompilerParams(collective_id=0, has_side_effects=True, vmem_limit_bytes=VMEM),
        )(x, dy, pre, w_in, w_down)
        dx, acc, down, _, full, _, dpre = out[:7]
        dw_in, dw_down, dx = finish(acc, full, dpre, down, dx)
        return dx, dw_in, dw_down

    rows = P(("dp", "tp"), None)
    cols = P("dp", "tp")
    return jax.shard_map(
        step, mesh=mesh,
        in_specs=(rows, rows, cols, P(None, "tp"), P("tp", None)),
        out_specs=(rows, cols, rows),
        check_vma=False,
    )
```

```python
import functools

import jax
import jax.numpy as jnp
import numpy as np
from jax import lax
from jax.experimental import pallas as pl
from jax.experimental.pallas import tpu as pltpu
from jax.sharding import PartitionSpec as P

MESH = pl.DeviceIdType.MESH
F32, BF16 = jnp.float32, jnp.bfloat16
D = 4096
FL = 1024
SH = 256
CHUNKS_A = ((0, 16, "p"), (16, 80, "q"), (96, 80, "q"), (176, 80, "q"))
CHUNKS_B = ((0, 128, "p"), (128, 64, "q"), (192, 64, "q"))
PR = 80
QR = 176
VMEM = 66_000_000
NT = (((1,), (1,)), ((), ()))
TN = (((0,), (0,)), ((), ()))


def dot(a, b, dims):
    return lax.dot_general(a, b, dims, preferred_element_type=F32)


def where_am_i():
    tp = lax.axis_index("tp")
    return tp // 8, (tp // 2) % 4, tp % 2


def tp_of(y, z, c):
    return y * 8 + z * 2 + c


def rdma(src, dst, ssem, rsem, dev):
    return pltpu.make_async_remote_copy(
        src_ref=src, dst_ref=dst, send_sem=ssem, recv_sem=rsem, device_id={"tp": dev}, device_id_type=MESH
    )


def greet(y, z, c):
    bar = pltpu.get_barrier_semaphore()

    def hello(dev):
        pl.semaphore_signal(bar, inc=1, device_id={"tp": dev}, device_id_type=MESH)

    hello(tp_of(y, z, 1 - c))
    hello(tp_of(1 - y, z, c))

    @pl.when(z > 0)
    def _():
        hello(tp_of(y, z - 1, c))

    @pl.when(z < 3)
    def _():
        hello(tp_of(y, z + 1, c))

    pl.semaphore_wait(bar, 2 + (z + 2) // 3 + (5 - z) // 3)


class Sends:
    def __init__(self):
        self.all = []

    def start(self, pred, make):
        self.all.append((pred, make))
        if pred is None:
            make().start()
        else:
            pl.when(pred)(lambda: make().start())

    def finish(self):
        for pred, make in self.all:
            if pred is None:
                make().wait_send()
            else:
                pl.when(pred)(lambda make=make: make().wait_send())


class Gather:
    def __init__(self, pos, own, full, rsem, zsem, ysem, sib_s, sib_r, chunks):
        self.y, self.z, self.c = pos
        self.own, self.full = own, full
        self.rsem, self.zsem, self.ysem, self.sib_s, self.sib_r = rsem, zsem, ysem, sib_s, sib_r
        self.chunks = chunks
        self.sends = Sends()

    def rows(self, y, z, k, c=None):
        r0, n = (0, SH) if k is None else self.chunks[k][:2]
        off = tp_of(y, z, self.c if c is None else c) * SH + r0
        return self.full.at[pl.ds(pl.multiple_of(off, 16), n)]

    def copy(self, dev, y, z, k, sems, own):
        r0, n, _ = self.chunks[k]
        src = self.own.at[pl.ds(r0, n)] if own else self.rows(y, z, k)
        d = y * 4 + z
        return rdma(src, self.rows(y, z, k), sems.at[d, k], self.rsem.at[d, k], dev)

    def send_z(self, step, y, z, k, pred=None, own=False):
        ok = self.z > 0 if step < 0 else self.z < 3
        if pred is not None:
            ok = jnp.logical_and(ok, pred)
        dev = tp_of(self.y, self.z + step, self.c)
        self.sends.start(ok, lambda: self.copy(dev, y, z, k, self.zsem.at[(step + 1) // 2], own))

    def send_y(self, y, z, k, pred=None, own=False):
        dev = tp_of(1 - self.y, self.z, self.c)
        self.sends.start(pred, lambda: self.copy(dev, y, z, k, self.ysem, own))

    def wait(self, y, z, k):
        self.copy(tp_of(1 - self.y, self.z, self.c), y, z, k, self.ysem, False).wait_recv()

    def sib_copy(self, y, z, c, own=False):
        d = y * 4 + z
        src = self.own if own else self.rows(y, z, None, c)
        return rdma(src, self.rows(y, z, None, c), self.sib_s.at[d], self.sib_r.at[d], tp_of(self.y, self.z, 1 - self.c))

    def send_sib(self, y, z, pred=None, own=False):
        self.sends.start(pred, lambda: self.sib_copy(y, z, self.c, own))

    def wait_sib(self, y, z):
        self.sib_copy(y, z, 1 - self.c).wait_recv()

    def begin_y(self):
        for k in range(len(self.chunks)):
            self.send_y(self.y, self.z, k, own=True)
        self.send_sib(self.y, self.z, own=True)

    def begin_z(self):
        for k in range(len(self.chunks)):
            self.send_z(1, self.y, self.z, k, own=True)
            self.send_z(-1, self.y, self.z, k, own=True)

    def turn(self):
        y, z = self.y, self.z
        for k, (_, _, kind) in enumerate(self.chunks):
            if kind == "p":
                self.wait(1 - y, z, k)
                self.send_z(1, 1 - y, z, k)
                self.send_z(-1, 1 - y, z, k)

    def step(self, s):
        y, z = self.y, self.z
        for k, (_, _, kind) in enumerate(self.chunks):
            for side in (-1, 1):
                zs = z + side * (s + 1)
                ok = zs >= 0 if side < 0 else zs <= 3
                for ys in (y, 1 - y) if kind == "p" else (y,):
                    pl.when(ok)(lambda ys=ys, zs=zs, k=k: self.wait(ys, zs, k))
                    if s < 2:
                        self.send_z(-side, ys, zs, k, pred=ok)
                if kind == "q":
                    self.send_y(y, zs, k, pred=ok)
        for side in (-1, 1):
            zs = z + side * (s + 1)
            self.send_sib(y, zs, pred=zs >= 0 if side < 0 else zs <= 3)

    def across(self, s):
        y, z = self.y, self.z
        for side in (-1, 1) if s else (0,):
            zs = z + side * s
            ok = None if s == 0 else zs >= 0 if side < 0 else zs <= 3

            def take(zs=zs):
                for k, (_, _, kind) in enumerate(self.chunks):
                    if kind == "q":
                        self.wait(1 - y, zs, k)

            if ok is None:
                take()
            else:
                pl.when(ok)(take)
            self.send_sib(1 - y, zs, pred=ok)


def local(src, dst, sem):
    return pltpu.make_async_copy(src, dst, sem)


def both(*copies):
    for cp in copies:
        cp.start()
    for cp in copies:
        cp.wait()


def kernel(x, dy, pre, w_in, w_down,
           dx, acc_o, dw_down, fy, fx, hidden, dpre, dps, wis, pl_b, pr_b, ps_b, ql_b, qr_b, qs_b, qy_b, qys_b, py_b, pys_b,
           wd_v, wo_v, ws_v, acc, big, blk, a1, a2, arr, obuf, pre_v, hid_v, dp_v,
           y_rs, y_zs, y_ys, y_ss, y_sr, x_rs, x_zs, x_ys, x_ss, x_sr,
           dps_s, dps_r, wis_sem, p_s, pl_r, pr_r, q_s, ql_r, qr_r, qy_s, qy_r, py_sem, lsem):
    y, z, c = where_am_i()
    greet(y, z, c)
    gy = Gather((y, z, c), dy, fy, y_rs, y_zs, y_ys, y_ss, y_sr, CHUNKS_A)
    gx = Gather((y, z, c), x, fx, x_rs, x_zs, x_ys, x_ss, x_sr, CHUNKS_B)
    gy.begin_y()
    gy.begin_z()
    other = tp_of(y, z, 1 - c)
    left, right, over = tp_of(y, z - 1, c), tp_of(y, z + 1, c), tp_of(1 - y, z, c)
    w_copy = rdma(w_in, wis, wis_sem.at[0], wis_sem.at[1], other)
    w_copy.start()
    load_w = local(w_down, wd_v, lsem.at[4])
    load_wo = local(w_in, wo_v, lsem.at[5])
    load_ws = local(wis, ws_v, lsem.at[6])
    load_w.start()
    load_wo.start()
    xv = big.at[pl.ds(0, 2 * SH)]

    def place_own(src, g):
        via = big.at[pl.ds(0, SH)]
        both(local(src, via, lsem.at[0]))
        both(local(via, g.rows(y, z, None), lsem.at[0]))

    def clear():
        def zero(m, _):
            acc[m // 4, pl.ds(pl.multiple_of((m % 4) * 256, 256), 256), :] = jnp.zeros((256, FL), F32)
            return 0

        lax.fori_loop(0, 16, zero, 0)

    def dps_copy(ys, zs):
        off = pl.multiple_of(tp_of(ys, zs, 1 - c) * SH, SH)
        d = ys * 4 + zs
        return rdma(dpre.at[pl.ds(off, SH)], dps.at[pl.ds(pl.multiple_of(d * SH, SH), SH)], dps_s.at[d], dps_r.at[d], other)


    def weigh():
        def weight(j, _):
            ms = pl.ds(pl.multiple_of((j % 4) * 256, 256), 256)
            cols = pl.ds(pl.multiple_of((j // 4) * FL, FL), FL)
            acc[j // 4, ms, :] += dot(hid_v[:, ms], big[0:512, cols], TN)
            return 0

        lax.fori_loop(0, 16, weight, 0)

    def chip_rows(ys, zs):
        return pl.ds(pl.multiple_of(tp_of(ys, zs, 0) * SH, SH), 2 * SH)

    def pair(ys, zs, pred=None, now=True):
        def go():
            gy.wait_sib(ys, zs)
            rows = chip_rows(ys, zs)
            both(local(fy.at[rows], xv, lsem.at[0]), local(pre.at[rows], pre_v, lsem.at[1]))

            def tile(j, _):
                cols = pl.ds(pl.multiple_of(j * 256, 256), 256)
                dh = dot(big[0:512, :], wd_v[cols, :], NT)
                p = pre_v[:, cols].astype(F32)
                k = np.float32(np.sqrt(2 / np.pi))
                t = jnp.tanh(k * (p + 0.044715 * (p * p * p)))
                cdf = 0.5 * (1.0 + t)
                slope = cdf + 0.5 * p * (1.0 - t * t) * (k * (1.0 + 3 * 0.044715 * (p * p)))
                hid_v[:, cols] = (p * cdf).astype(BF16)
                dp_v[:, cols] = (dh * slope).astype(BF16)
                return 0

            lax.fori_loop(0, FL // 256, tile, 0)
            out = local(dp_v, dpre.at[rows], lsem.at[3])
            if now:
                out.start()
                weigh()
                out.wait()
            else:
                both(out, local(hid_v, hidden.at[rows], lsem.at[2]))
            dps_copy(ys, zs).start()

        if pred is None:
            go()
        else:
            pl.when(pred)(go)

    def early(ys, zs, pred):
        pair(ys, zs, pred, now=False)

    def late(ys, zs):
        rows = chip_rows(ys, zs)
        both(local(fy.at[rows], xv, lsem.at[0]), local(hidden.at[rows], hid_v, lsem.at[1]))
        weigh()

    def pairs(do, s, flip):
        def one(i, _):
            zs = z + (2 * i - 1) * s
            do(1 - y if flip else y, zs, jnp.logical_and(zs >= 0, zs <= 3))
            return 0

        lax.fori_loop(0, 2, one, 0)

    place_own(dy, gy)
    clear()
    load_w.wait()
    gy.turn()
    pair(y, z)
    gy.step(0)
    gy.across(0)
    pair(1 - y, z)
    pairs(pair, 1, False)
    gy.step(1)
    gx.begin_z()
    place_own(x, gx)
    gy.across(1)
    pairs(early, 1, True)
    gy.step(2)
    gx.begin_y()
    pairs(early, 2, False)
    gy.across(2)
    pairs(early, 2, True)
    pairs(early, 3, False)
    w_copy.wait()
    load_ws.start()
    gy.across(3)
    pairs(early, 3, True)


    inner = jnp.logical_and(z > 0, z < 3)
    outer = jnp.logical_not(inner)
    high = z // 2
    inward = 1 - 2 * high
    far = high * z + (1 - high) * (3 - z)

    def target(i):
        o = (0, 1, 5 - far, far)[i]
        return high * o + (1 - high) * (3 - o)

    def fetch(ys, zs, r0, n, at, sem=0):
        o = pl.multiple_of(tp_of(ys, zs, c) * SH + r0, 16)
        s = pl.multiple_of((ys * 4 + zs) * SH + r0, 16)
        return (local(dpre.at[pl.ds(o, n)], a1.at[pl.ds(at, n)], lsem.at[sem]),
                local(dps.at[pl.ds(s, n)], a2.at[pl.ds(at, n)], lsem.at[sem + 1]))

    def fetch_all(parts):
        for part in parts:
            both(*part)

    def cols512(j):
        return pl.ds(pl.multiple_of(j * 512, 512), 512)

    def q_terms():
        fetch_all([fetch(1 - y, target(i), PR, QR, i * QR) for i in range(4)])

        def tile(j, _):
            cols = cols512(j)
            big[:, cols] = (dot(a1[...], wo_v[cols, :], NT) + dot(a2[...], ws_v[cols, :], NT)).astype(BF16)
            return 0

        lax.fori_loop(0, D // 512, tile, 0)
        both(*(local(big.at[pl.ds(i * QR, QR)], qys_b.at[target(i)], lsem.at[i]) for i in range(4)))

    def terms(v):
        both(*fetch(1 - y, v, 0, PR, 0), *fetch(y, v, 0, SH, PR, 2))
        n = PR + SH

        def tile(j, _):
            cols = cols512(j)
            blk[:, cols] = dot(a1[0:n, :], wo_v[cols, :], NT) + dot(a2[0:n, :], ws_v[cols, :], NT)
            return 0

        lax.fori_loop(0, D // 512, tile, 0)

    def add(buf, copy, at, n):
        copy.wait_recv()
        both(local(buf, arr.at[pl.ds(0, n)], lsem.at[2]))

        def tile(j, _):
            cols = cols512(j)
            blk[at:at + n, cols] += arr[0:n, cols].astype(F32)
            return 0

        lax.fori_loop(0, D // 512, tile, 0)

    def store(buf, at, n):
        def tile(j, _):
            cols = cols512(j)
            obuf[0:n, cols] = blk[at:at + n, cols].astype(BF16)
            return 0

        lax.fori_loop(0, D // 512, tile, 0)
        both(local(obuf.at[pl.ds(0, n)], buf, lsem.at[3]))

    def p_copy(ys, v, dev, rightward):
        i = ys * 4 + v
        dst, sem = (pl_b, pl_r) if rightward else (pr_b, pr_r)
        return rdma(ps_b.at[i], dst.at[i], p_s.at[i], sem.at[i], dev)

    def q_copy(v, dev, rightward):
        dst, sem = (ql_b, ql_r) if rightward else (qr_b, qr_r)
        return rdma(qs_b.at[v], dst.at[v], q_s.at[v], sem.at[v], dev)

    def qy_copy(v):
        return rdma(qys_b.at[v], qy_b.at[v], qy_s.at[v], qy_r.at[v], over)

    def py_copy():
        return rdma(pys_b, py_b, py_sem.at[0], py_sem.at[1], over)

    def from_left(ok, ys, v, at):
        if ys is None:
            pl.when(ok)(lambda: add(ql_b.at[v], q_copy(v, right, True), at, QR))
        else:
            pl.when(ok)(lambda: add(pl_b.at[ys * 4 + v], p_copy(ys, v, right, True), at, PR))

    def from_right(ok, ys, v, at):
        if ys is None:
            pl.when(ok)(lambda: add(qr_b.at[v], q_copy(v, left, False), at, QR))
        else:
            pl.when(ok)(lambda: add(pr_b.at[ys * 4 + v], p_copy(ys, v, left, False), at, PR))

    def towards(i, pred, fill=(None, None)):
        v = target(i)
        up, down = v > z, v < z

        def go():
            terms(v)
            for ys, at, other_work in ((1 - y, 0, fill[0]), (y, PR, fill[1])):
                from_left(jnp.logical_and(inner, up), ys, v, at)
                from_right(jnp.logical_and(inner, down), ys, v, at)
                store(ps_b.at[ys * 4 + v], at, PR)
                pl.when(up)(lambda ys=ys: p_copy(ys, v, right, True).start())
                pl.when(down)(lambda ys=ys: p_copy(ys, v, left, False).start())
                if other_work is not None:
                    other_work()
            add(qy_b.at[v], qy_copy(v), 2 * PR, QR)
            from_left(jnp.logical_and(inner, up), None, v, 2 * PR)
            from_right(jnp.logical_and(inner, down), None, v, 2 * PR)
            store(qs_b.at[v], 2 * PR, QR)
            pl.when(up)(lambda: q_copy(v, right, True).start())
            pl.when(down)(lambda: q_copy(v, left, False).start())

        pl.when(pred)(go)

    def arrived(ys, at):
        from_left(z > 0, ys, z, at)
        from_right(z < 3, ys, z, at)

    def in_step(ys, zs, pred=None):
        def go():
            gx.wait_sib(ys, zs)
            rows = chip_rows(ys, zs)
            both(local(fx.at[rows], xv, lsem.at[0]), local(dpre.at[rows], dp_v, lsem.at[1]))

            def row(m, _):
                here = pl.ds(pl.multiple_of((m % 4) * 256, 256), 256)
                acc[m // 4, here, :] += dot(big[0:512, pl.ds(pl.multiple_of(m * 256, 256), 256)], dp_v[...], TN)
                return 0

            lax.fori_loop(0, D // 256, row, 0)

        if pred is None:
            go()
        else:
            pl.when(pred)(go)

    def write(to):
        def one(m, _):
            h0, h1 = pl.ds(0, 512), pl.ds(512, 512)
            hid_v[...] = acc[m, h0, :].astype(BF16)
            first = local(hid_v, to(m, 0), lsem.at[0])
            first.start()
            pre_v[...] = acc[m, h1, :].astype(BF16)
            both(local(pre_v, to(m, 1), lsem.at[1]))
            first.wait()
            return 0

        lax.fori_loop(0, 4, one, 0)

    for d in range(8):
        cp = rdma(dpre.at[pl.ds(0, SH)], dps.at[pl.ds(d * SH, SH)], dps_s.at[d], dps_r.at[d], other)
        cp.wait_recv()
        cp.wait_send()
    gx.turn()
    load_wo.wait()
    load_ws.wait()
    q_terms()
    qy_copy(target(0)).start()
    qy_copy(target(1)).start()
    towards(0, outer)
    gx.step(0)

    def late_first(k, _):
        late(jnp.where(inner, 1 - y, jnp.where(k == 0, 1 - y, y)), z + inward * jnp.where(inner, 1 - 2 * k, 1 + k))
        return 0

    def late_rest(k, _):
        late(jnp.where(k % 2 == 0, 1 - y, y), z + inward * (1 + (k + 1) // 2))
        return 0

    lax.fori_loop(0, 2, late_first, 0)
    gx.across(0)
    qy_copy(target(2)).start()
    towards(0, inner, (lambda: late(y, z + 2 * inward), lambda: late(1 - y, z + 2 * inward)))
    towards(1, outer)
    gx.step(1)
    qy_copy(target(3)).start()
    lax.fori_loop(2, jnp.where(inner, 2, 5), late_rest, 0)
    write(lambda m, h: dw_down.at[pl.ds(h * 512, 512), pl.ds(pl.multiple_of(m * FL, FL), FL)])
    clear()
    in_step(y, z)
    in_step(1 - y, z, outer)
    towards(1, inner, (lambda: in_step(1 - y, z), lambda: in_step(y, z - 1)))
    towards(2, outer)
    gx.across(1)
    gx.step(2)
    towards(2, inner)

    def pass_over():
        terms(z)
        arrived(1 - y, 0)
        store(pys_b, 0, PR)
        py_copy().start()

    in_step(y, jnp.where(inner, z + 1, z + inward))
    pl.when(inner)(pass_over)
    pairs(in_step, 1, True)
    pl.when(outer)(pass_over)
    gx.across(2)
    in_step(y, z + 2 * inward, outer)
    in_step(1 - y, z + 2 * inward, outer)
    save = local(acc, acc_o, lsem.at[4])
    save.start()
    terms(z)
    add(qy_b.at[z], qy_copy(z), 2 * PR, QR)
    arrived(None, 2 * PR)
    store(dx.at[pl.ds(PR, QR)], 2 * PR, QR)
    arrived(y, PR)
    add(py_b, py_copy(), PR, PR)
    store(dx.at[pl.ds(0, PR)], PR, PR)
    gx.across(3)
    gx.wait_sib(y, 3 - 3 * high)
    gx.wait_sib(1 - y, 3 - 3 * high)
    save.wait()

    for i in range(3):
        v = target(i)
        for ys in (1 - y, y):
            p_copy(ys, v, left, False).wait_send()
        q_copy(v, left, False).wait_send()
    for i in range(4):
        qy_copy(target(i)).wait_send()
    py_copy().wait_send()
    gy.sends.finish()
    gx.sends.finish()


def place(acc, x0, x1, dp0, dp1, down_in, dx_in, dw_in, down, dx):
    total = acc[...] + dot(x0[...], dp0[...], TN) + dot(x1[...], dp1[...], TN)
    dw_in[...] = total.astype(BF16)
    down[...] = down_in[...]
    dx[...] = dx_in[...]


def finish(acc, full, dpre, down, dx):
    def chip(other):
        tp = lax.axis_index("tp")
        y = tp // 8
        return (1 - y if other else y) * 4 + 3 - 3 * ((tp // 2) % 4 // 2)

    steps = 8
    tall = pl.BlockSpec((FL // steps, D), lambda i: (i, 0))
    flat = pl.BlockSpec((SH // steps, D), lambda i: (i, 0))
    part = pl.BlockSpec((D // steps, FL), lambda i: (i, 0))
    return pl.pallas_call(
        place,
        name="finish",
        grid=(steps,),
        in_specs=[
            part,
            pl.BlockSpec((2 * SH, D // steps), lambda i: (chip(False), i)),
            pl.BlockSpec((2 * SH, D // steps), lambda i: (chip(True), i)),
            pl.BlockSpec((2 * SH, FL), lambda i: (chip(False), 0)),
            pl.BlockSpec((2 * SH, FL), lambda i: (chip(True), 0)),
            tall, flat,
        ],
        out_specs=[part, tall, flat],
        out_shape=[jax.ShapeDtypeStruct(s, BF16) for s in ((D, FL), (FL, D), (SH, D))],
        compiler_params=pltpu.CompilerParams(vmem_limit_bytes=VMEM),
    )(acc.reshape(D, FL), full, full, dpre, dpre, down, dx)


def solution(mesh):
    any_ = pl.BlockSpec(memory_space=pl.ANY)
    dma = pltpu.SemaphoreType.DMA

    def arr(*shape):
        return jax.ShapeDtypeStruct(shape, BF16)

    def vmem(*shape, dtype=BF16):
        return pltpu.VMEM(shape, dtype)

    gather_sems = [dma((8, 4)), dma((2, 8, 4)), dma((8, 4)), dma((8,)), dma((8,))]

    def step(x, dy, pre, w_in, w_down):
        outs = [
            arr(SH, D), jax.ShapeDtypeStruct((4, FL, FL), F32), arr(FL, D), arr(D, D), arr(D, D),
            arr(D, FL), arr(D, FL), arr(8 * SH, FL), arr(D, FL),
            arr(8, PR, D), arr(8, PR, D), arr(8, PR, D),
            arr(4, QR, D), arr(4, QR, D), arr(4, QR, D), arr(4, QR, D), arr(4, QR, D),
            arr(PR, D), arr(PR, D),
        ]
        out = pl.pallas_call(
            kernel,
            name="backward",
            out_shape=outs,
            in_specs=[any_] * 5,
            out_specs=[any_] * len(outs),
            scratch_shapes=[
                vmem(FL, D), vmem(D, FL), vmem(D, FL), vmem(4, FL, FL, dtype=F32), vmem(4 * QR, D),
                vmem(PR + SH, D, dtype=F32), vmem(4 * QR, FL), vmem(4 * QR, FL), vmem(QR, D), vmem(QR, D),
                vmem(2 * SH, FL), vmem(2 * SH, FL), vmem(2 * SH, FL),
                *gather_sems, *gather_sems, dma((8,)), dma((8,)), dma((2,)),
                dma((8,)), dma((8,)), dma((8,)), dma((4,)), dma((4,)), dma((4,)), dma((4,)), dma((4,)), dma((2,)), dma((7,)),
            ],
            compiler_params=pltpu.CompilerParams(collective_id=0, has_side_effects=True, vmem_limit_bytes=VMEM),
        )(x, dy, pre, w_in, w_down)
        dx, acc, down, _, full, _, dpre = out[:7]
        dw_in, dw_down, dx = finish(acc, full, dpre, down, dx)
        return dx, dw_in, dw_down

    rows = P(("dp", "tp"), None)
    cols = P("dp", "tp")
    return jax.shard_map(
        step, mesh=mesh,
        in_specs=(rows, rows, cols, P(None, "tp"), P("tp", None)),
        out_specs=(rows, cols, rows),
        check_vma=False,
    )
```
